256 devices in a mesh: wide: 32 (over z_hi, y, core), shard: 8 (over z_lo, x).
Axes of the slice: x: 4, y: 4, z: 8 (z_hi: 4, z_lo: 2; z = z_hi * 2 + z_lo), core: 2. Of those that a mesh axis runs over, the one named last changes fastest.
Arguments:
- weights: bfloat16 [1024, 8192], P('shard'), may hold values from -6 to 6
- momentum: bfloat16 [32, 1024, 8192], P('wide', 'shard'), may hold values from -6 to 6
- grads: bfloat16 [2, 32, 1024, 8192], P(None, 'wide', 'shard'), may hold values from -6 to 6
- offsets: int32 [8, 64], P('shard'), may hold values from 0 to 96
- owners: int32 [8, 64], P('shard'), may hold values from 0 to 63, each once within a row
- exp_avg: float32 [8, 64, 32, 128], P('shard', 'wide'), may hold values from -7 to 7
- exp_sq: float32 [8, 64, 32, 128], P('shard', 'wide'), may hold values from 0.01 to 1
Outputs:
- new_weights: bfloat16 [1024, 8192], P('shard')
- new_momentum: bfloat16 [32, 1024, 8192], P('wide', 'shard')
- new_avg: float32 [8, 64, 32, 128], P('shard', 'wide')
- new_sq: float32 [8, 64, 32, 128], P('shard', 'wide')
- scales: float32 [2], replicated
The draws below stay inside these ranges and needn't reach their ends.
Inputs may be any that keep to these rules, and one draw needn't show every extreme that they name: `offsets`: each block's band spans 32 consecutive transform rows. Each row of owners is a permutation of 0 to 63.
All inputs are finite; a program needn't handle non-finite values.
Results may differ from the reference program's by a relative error of at most 0.003.
Values may be sent and summed in bfloat16 or wider, within the bound.
A program may use at most 128 MiB of HBM per device.

```python
import math
import jax
import jax.numpy as jnp
from jax import lax

BLOCK = 128
BAND = 32
COLS = 8192
STEPS = 2
ROW_BLOCKS = 8
ROWS = 1024
CB = 64
REPLICAS = 32


def draw_exp_avg(key, part):
    array_shape = (ROW_BLOCKS, CB, BAND, BLOCK)
    row_pos = jnp.arange(ROW_BLOCKS, dtype=jnp.float32)[:, None, None, None] / max(ROW_BLOCKS - 1, 1)
    slot_pos = jnp.arange(CB, dtype=jnp.float32)[None, :, None, None] / max(CB - 1, 1)
    scaling = 0.15 * 3.0 ** (row_pos + slot_pos)
    base_draw = jnp.clip(jax.random.normal(key, array_shape, jnp.float32), -4.0, 4.0)
    return base_draw * scaling


def touch_ends(array, key, smallest, largest):
    extent = array.shape
    spot = [jax.random.randint(jax.random.fold_in(key, axis), (), 0, extent[axis]) for axis in range(len(extent))]
    array = array.at[tuple(spot)].set(smallest)
    longest = extent.index(max(extent))
    spot[longest] = (spot[longest] + 1) % extent[longest]
    return array.at[tuple(spot)].set(largest)


def raised(entries, key, source, target, parts, factor):
    owner, partner = [(jnp.arange(entries.shape[dim]) // (entries.shape[dim] // parts)).reshape([-1 if axis == dim else 1 for axis in range(entries.ndim)]) for dim in (source, target)]
    chosen = jax.random.permutation(key, parts)[partner]
    strong = (owner == chosen) | (owner == (partner + parts // 2) % parts)
    return jnp.where(strong, factor * entries, entries)


def steps_of(rng, dims, shards, low, high):
    loudness, own = 1.0, jax.random.fold_in(rng, 6)
    for dim, blocks in shards:
        draws = jnp.exp(jax.random.uniform(jax.random.fold_in(own, dim), (blocks,), jnp.float32, low / len(shards), high / len(shards)))
        loudness = loudness * jnp.repeat(draws, dims[dim] // blocks).reshape([-1 if axis == dim else 1 for axis in range(len(dims))])
    return loudness


def scatter_about(own_key, shape, deviation, bound, pieces=(), kind=jnp.bfloat16):
    entries = jax.random.normal(own_key, shape, jnp.float32) * deviation
    if len(pieces) > 0:
        entries = steps_of(own_key, shape, pieces, -0.22, 0.18) * entries
    return jnp.clip(entries, min=-bound, max=bound).astype(kind)


def heavy_noise(own_key, extent, scale, limit, pieces, heavy, kind=jnp.bfloat16):
    values = scale * jax.random.normal(own_key, extent, jnp.float32)
    if pieces:
        values = values * steps_of(own_key, extent, pieces, -0.22, 0.18)
    return jnp.clip(raised(values, jax.random.fold_in(own_key, 3), *heavy), -limit, limit).astype(kind)


def setup_inputs(seed: int = 0) -> dict:
    keys = jax.random.split(jax.random.key(seed), 8)
    return {
        "weights": scatter_about(keys[0], (ROWS, COLS), 1.0, 6.0, ((0, 8),)),
        "momentum": scatter_about(keys[1], (REPLICAS, ROWS, COLS), 1.0, 6.0, ((0, 32), (1, 8))),
        "grads": heavy_noise(keys[2], (STEPS, REPLICAS, ROWS, COLS), 1.0, 6.0, ((1, 32), (2, 8)), (1, 3, 32, 2.75)),
        "offsets": touch_ends(jax.random.randint(keys[3], (ROW_BLOCKS, CB), 0, BLOCK - BAND + 1), jax.random.fold_in(keys[3], 1), 0, BLOCK - BAND).astype(jnp.int32),
        "owners": jax.vmap(lambda own: jax.random.permutation(own, CB))(jax.random.split(keys[4], ROW_BLOCKS)).reshape((ROW_BLOCKS, CB)).astype(jnp.int32),
        "exp_avg": draw_exp_avg(jax.random.fold_in(keys[7], 71), 0),
        "exp_sq": jnp.clip(jnp.exp(math.log(1.0) - 4.6051702 * jax.random.uniform(keys[6], (ROW_BLOCKS, CB, BAND, BLOCK), jnp.float32) ** steps_of(keys[6], (ROW_BLOCKS, CB, BAND, BLOCK), ((0, 8), (1, 32)), -0.2, 0.2)), 0.01, 1.0),
    }


highest = lax.Precision.HIGHEST
momentum_decay = 0.9
beta_one = 0.8
beta_two = 0.95
adam_eps = 1e-08
rms_eps = 1e-06
learning_rate = 0.2

def dct_table(length):
    frequency = jnp.arange(length, dtype=jnp.float32)[:, None]
    position = jnp.arange(length, dtype=jnp.float32)[None, :]
    cosines = jnp.cos(jnp.pi * (2.0 * position + 1.0) * frequency / (2.0 * length))
    scaling = jnp.where(frequency == 0.0, jnp.sqrt(1.0 / length), jnp.sqrt(2.0 / length))
    return cosines * scaling

def band_tables(basis, offsets):
    indices = offsets[:, :, None] + jnp.arange(BAND, dtype=jnp.int32)[None, None, :]
    return basis[indices]

def forward(blended, picked, basis):
    left_part = jnp.einsum('rjpa,rajb->rjpb', picked, blended, precision=highest)
    return jnp.einsum('rjpb,cb->rjpc', left_part, basis, precision=highest)

def inverse(coefs, picked, basis):
    right_part = jnp.einsum('rjpc,cb->rjpb', coefs, basis, precision=highest)
    return jnp.einsum('rjpa,rjpb->rajb', picked, right_part, precision=highest)

def reference(weights, momentum, grads, offsets, owners, exp_avg, exp_sq):
    basis = dct_table(BLOCK)
    picked = band_tables(basis, offsets)
    slot_order = jnp.argsort(owners, axis=1).astype(jnp.int32)
    block_shape = (ROW_BLOCKS, BLOCK, CB, BLOCK)
    weight_now = weights.astype(jnp.float32).reshape(block_shape)
    moment_now = momentum.astype(jnp.float32).reshape((REPLICAS,) + block_shape)
    avg_now = exp_avg
    sq_now = exp_sq
    scales = []
    for step_index in range(STEPS):

        def one_replica(pair_in):
            held_moment, grad_now = pair_in
            blended = momentum_decay * held_moment + grad_now.astype(jnp.float32).reshape(block_shape)
            band_coef = forward(blended, picked, basis)
            return (band_coef, blended - inverse(band_coef, picked, basis))
        bands, moment_now = lax.map(one_replica, (moment_now, grads[step_index]))
        mean_band = lax.optimization_barrier(jnp.sum(bands, axis=0)) / REPLICAS
        slot_band = jnp.take_along_axis(mean_band, slot_order[:, :, None, None], axis=1)
        avg_now = beta_one * avg_now + (1.0 - beta_one) * slot_band
        sq_now = beta_two * sq_now + (1.0 - beta_two) * slot_band * slot_band
        raw_update = avg_now / (jnp.sqrt(sq_now) + adam_eps)
        spread = jnp.sqrt(jnp.mean(raw_update * raw_update) + rms_eps)
        update = (raw_update / spread).astype(jnp.bfloat16)
        block_update = jnp.take_along_axis(update.astype(jnp.float32), owners[:, :, None, None], axis=1)
        weight_now = weight_now - learning_rate * inverse(block_update, picked, basis)
        scales.append(spread)
    new_weights = weight_now.reshape(ROWS, COLS).astype(jnp.bfloat16)
    new_momentum = moment_now.reshape(REPLICAS, ROWS, COLS).astype(jnp.bfloat16)
    return (new_weights, new_momentum, avg_now, sq_now, jnp.stack(scales))
```

```python
import functools

import jax
import jax.numpy as jnp
import numpy as np
from jax import lax
from jax.experimental import pallas as pl
from jax.experimental.pallas import tpu as pltpu
from jax.sharding import Mesh
from jax.sharding import PartitionSpec as P

STEPS = 2
BLOCK = 128
BAND = 32
CHUNKS = 8
WIDE = ("zh", "y", "c")
SHARD = ("zl", "x")
MESH = pl.DeviceIdType.MESH
F32 = jnp.float32
BF16 = jnp.bfloat16

momentum_decay = 0.9
beta_one = 0.8
beta_two = 0.95
adam_eps = 1e-08
rms_eps = 1e-06
learning_rate = 0.2


def dct_table(length):
    k = np.arange(length, dtype=np.float64)[:, None]
    n = np.arange(length, dtype=np.float64)[None, :]
    table = np.cos(np.pi * (2.0 * n + 1.0) * k / (2.0 * length))
    return (table * np.where(k == 0.0, np.sqrt(1.0 / length), np.sqrt(2.0 / length))).astype(np.float32)


def split(value):
    high = value.astype(BF16)
    return high, (value - high.astype(F32)).astype(BF16)


def tall(table):
    high = table.astype(BF16)
    low = (table - high.astype(np.float32)).astype(BF16)
    return np.concatenate([high, high, low], axis=0)


def wide_lhs(value):
    high, low = split(value)
    return jnp.concatenate([high, low, high], axis=-1)


def dot(a, b):
    return jnp.dot(a, b, preferred_element_type=F32)


def project_back(rows, coefs):
    p_high, p_low = split(rows)
    q_high, q_low = split(coefs)
    left = jnp.concatenate([p_high, p_low, p_high], axis=0)
    right = jnp.concatenate([q_high, q_high, q_low], axis=0)
    return lax.dot_general(left, right, (((0,), (0,)), ((), ())), preferred_element_type=F32)


def main_kernel(
    offs, order, basis_in, tall_in, mom_in, grad_in, avg_in, sq_in,
    mom_out, gathered, avg_out, sq_out, spread_out,
    mbuf, gbuf, left, band, csend, crecv, ysend, yone, ytwo, zsend, zrecv, own,
    tot_one, tot_two, tot_three, got_one, got_two, got_three,
    load_sem, c_sem, y_sem, z_sem, az_sem, ay_sem, ac_sem, s_sem,
):
    zh, y, c = lax.axis_index("zh"), lax.axis_index("y"), lax.axis_index("c")
    zl, x = lax.axis_index("zl"), lax.axis_index("x")
    n_cb = left.shape[0]
    per = n_cb // CHUNKS
    y_up, y_down = {"y": lax.rem(y + 1, 4)}, {"y": lax.rem(y + 3, 4)}
    other = {"c": 1 - c}

    def zh_at(q):
        return {"zh": lax.rem(zh + q, 4)}

    one_peers = [
        {"zl": lax.rem(zl + i, 2), "x": lax.rem(x + j, 4)} for i in range(2) for j in range(4) if i or j
    ]
    two_peers = [
        {"c": lax.rem(c + i, 2), "y": lax.rem(y + j, 4)} for i in range(2) for j in range(4) if i or j
    ]
    three_peers = [zh_at(q) for q in (1, 2, 3)]

    def load(chunk):
        cols = pl.ds(pl.multiple_of(chunk * (per * BLOCK), 128), per * BLOCK)
        return (
            pltpu.make_async_copy(mom_in.at[0, :, cols], mbuf.at[chunk], load_sem.at[0, chunk]),
            pltpu.make_async_copy(grad_in.at[0, 0, :, cols], gbuf.at[0, chunk], load_sem.at[1, chunk]),
            pltpu.make_async_copy(grad_in.at[1, 0, :, cols], gbuf.at[1, chunk], load_sem.at[2, chunk]),
        )

    def start_load(chunk, _):
        for copy in load(chunk):
            copy.start()
        return 0

    lax.fori_loop(0, CHUNKS, start_load, 0)

    barrier = pltpu.get_barrier_semaphore()
    everyone = one_peers + two_peers + three_peers
    for peer in everyone:
        pl.semaphore_signal(barrier, inc=1, device_id=peer, device_id_type=MESH)

    def bands(chunk, _):
        for copy in load(chunk):
            copy.wait()
        for i in range(per):
            j = chunk * per + i
            cols = slice(i * BLOCK, (i + 1) * BLOCK)
            rows = basis_in[pl.ds(offs[j], BAND), :]
            both = jnp.concatenate(split(rows), axis=0)
            m = dot(both, mbuf[chunk, :, cols])
            g = dot(both, gbuf[0, chunk, :, cols])
            h = dot(both, gbuf[1, chunk, :, cols])
            left[j, 0] = momentum_decay * (m[:BAND] + m[BAND:]) + (g[:BAND] + g[BAND:])
            left[j, 1] = h[:BAND] + h[BAND:]
        value = left[pl.ds(chunk * per, per)].reshape(per * STEPS * BAND, BLOCK)
        out = dot(wide_lhs(value), tall_in[...])
        band[pl.ds(chunk * per, per)] = out.astype(BF16).reshape(per, STEPS, BAND, BLOCK)
        return 0

    lax.fori_loop(0, CHUNKS, bands, 0)

    def slot(r, k, q, core):
        return lax.rem(zh + q, 4) * 16 + lax.rem(y + r, 4) * 4 + core * 2 + k

    def pack(r):
        def body(i, _):
            k, q = i // 4, lax.rem(i, 4)
            csend[r, k, q] = band[order[slot(r, k, q, 1 - c)]]
            return 0

        lax.fori_loop(0, 8, body, 0)

    def remote(src, dst, sems, index, peer):
        return pltpu.make_async_remote_copy(
            src_ref=src, dst_ref=dst, send_sem=sems.at[(0,) + index], recv_sem=sems.at[(1,) + index],
            device_id=peer, device_id_type=MESH,
        )

    sends = []

    def start(copy):
        copy.start()
        sends.append(copy)
        return copy

    ranks = (2, 1, 3, 0)
    c_copies = {}
    pack(2)
    pl.semaphore_wait(barrier, len(everyone))
    for r in ranks:
        if r != 2:
            pack(r)
        c_copies[r] = start(remote(csend.at[r], crecv.at[r], c_sem, (r,), other))

    def merge(r):
        def body(i, _):
            k, q = i // 4, lax.rem(i, 4)
            total = band[order[slot(r, k, q, c)]].astype(F32) + crecv[r, k, q].astype(F32)
            if r == 0:
                own[k, q] = total
            else:
                ysend[r - 1, k, q] = total.astype(BF16)
            return 0

        lax.fori_loop(0, 8, body, 0)

    q_order = (2, 1, 3, 0)
    c_copies[2].wait_recv()
    merge(2)
    first = {}
    for q in q_order:
        first[0, q] = start(remote(ysend.at[1, 0, q], yone.at[0, q], y_sem, (0, q), y_up))
        first[1, q] = start(remote(ysend.at[1, 1, q], yone.at[1, q], y_sem, (1, q), y_down))
    c_copies[1].wait_recv()
    merge(1)
    c_copies[3].wait_recv()
    merge(3)
    early = {}
    for q in q_order:
        early[0, q] = start(remote(ysend.at[0, 1, q], ytwo.at[0, 1, q], y_sem, (2, q), y_up))
        early[1, q] = start(remote(ysend.at[2, 0, q], ytwo.at[1, 0, q], y_sem, (3, q), y_down))
    c_copies[0].wait_recv()
    merge(0)
    late = {}
    for q in q_order:
        first[0, q].wait_recv()
        ysend[0, 0, q] = (ysend[0, 0, q].astype(F32) + yone[0, q].astype(F32)).astype(BF16)
        late[0, q] = start(remote(ysend.at[0, 0, q], ytwo.at[0, 0, q], y_sem, (4, q), y_up))
        first[1, q].wait_recv()
        ysend[2, 1, q] = (ysend[2, 1, q].astype(F32) + yone[1, q].astype(F32)).astype(BF16)
        late[1, q] = start(remote(ysend.at[2, 1, q], ytwo.at[1, 1, q], y_sem, (5, q), y_down))

    def momenta(chunk, _):
        for i in range(per):
            j = chunk * per + i
            cols = slice(i * BLOCK, (i + 1) * BLOCK)
            rows = basis_in[pl.ds(offs[j], BAND), :]
            lost = project_back(rows, momentum_decay * left[j, 0] + left[j, 1])
            blended = momentum_decay * mbuf[chunk, :, cols].astype(F32) + gbuf[0, chunk, :, cols].astype(F32)
            blended = momentum_decay * blended + gbuf[1, chunk, :, cols].astype(F32)
            where = pl.ds(pl.multiple_of(j * BLOCK, 128), BLOCK)
            mom_out[0, :, where] = (blended - lost).astype(BF16)
        return 0

    lax.fori_loop(0, CHUNKS // 2, momenta, 0)

    z_copies = {}
    for q in q_order:
        for copies in (early, late):
            copies[0, q].wait_recv()
            copies[1, q].wait_recv()
        for k in range(2):
            total = own[k, q] + ytwo[0, k, q].astype(F32) + ytwo[1, k, q].astype(F32)
            if q == 0:
                own[k, 0] = total
            else:
                zsend[q - 1, k] = total.astype(BF16)
        if q != 0:
            z_copies[q] = start(remote(zsend.at[q - 1], zrecv.at[q - 1], z_sem, (q - 1,), zh_at(q)))

    lax.fori_loop(CHUNKS // 2, CHUNKS, momenta, 0)

    for q in (1, 3, 2):
        z_copies[q].wait_recv()
    base = zh * 16 + y * 4 + c * 2
    tot_one[...] = jnp.zeros_like(tot_one)
    replicas = lax.axis_size("zh") * lax.axis_size("y") * lax.axis_size("c")
    for k in range(2):
        mean = own[k, 0] + zrecv[0, k].astype(F32) + zrecv[1, k].astype(F32) + zrecv[2, k].astype(F32)
        mean = mean * (1.0 / replicas)
        avg, sq = avg_in[0, k], sq_in[0, k]
        for step in range(STEPS):
            avg = beta_one * avg + (1.0 - beta_one) * mean[step]
            sq = beta_two * sq + (1.0 - beta_two) * mean[step] * mean[step]
            raw = avg / (jnp.sqrt(sq) + adam_eps)
            gathered[base + k, step] = raw.astype(BF16)
            tot_one[step] += jnp.sum((raw * raw).reshape(BAND // 8, 8, BLOCK), axis=0)
        avg_out[0, k] = avg
        sq_out[0, k] = sq

    def block(q, r, core):
        return lax.rem(zh + q, 4) * 16 + lax.rem(y + r, 4) * 4 + core * 2

    mine = gathered.at[pl.ds(base, 2)]
    for q in (2, 1, 3):
        start(remote(mine, mine, az_sem, (q - 1,), zh_at(q)))
    for i, peer in enumerate(one_peers):
        start(remote(tot_one, got_one.at[i], s_sem, (i,), peer))

    def arrived(view, sems, index, peer):
        remote(view, view, sems, index, peer).wait_recv()

    def to_partner(view, index):
        start(remote(view, view, ac_sem, index, other))

    def y_start(q):
        view = gathered.at[pl.ds(block(q, 0, c), 2)]
        start(remote(view, view, ay_sem, (0, q), y_up))
        start(remote(view, view, ay_sem, (1, q), y_down))
        to_partner(view, (0, q))

    def y_forward(q):
        view = gathered.at[pl.ds(block(q, 3, c), 2)]
        arrived(view, ay_sem, (0, q), y_up)
        half = gathered.at[pl.ds(block(q, 3, c), 1)]
        start(remote(half, half, ay_sem, (2, q), y_up))
        to_partner(view, (1, q))
        view = gathered.at[pl.ds(block(q, 1, c), 2)]
        arrived(view, ay_sem, (1, q), y_down)
        half = gathered.at[pl.ds(block(q, 1, c) + 1, 1)]
        start(remote(half, half, ay_sem, (3, q), y_down))
        to_partner(view, (2, q))

    def y_finish(q):
        half = gathered.at[pl.ds(block(q, 2, c), 1)]
        arrived(half, ay_sem, (2, q), y_up)
        to_partner(half, (3, q))
        half = gathered.at[pl.ds(block(q, 2, c) + 1, 1)]
        arrived(half, ay_sem, (3, q), y_down)
        to_partner(half, (4, q))

    def z_arrived(q):
        view = gathered.at[pl.ds(block(q, 0, c), 2)]
        arrived(view, az_sem, (4 - q - 1,), zh_at(q))
        y_start(q)

    y_start(0)
    z_arrived(1)
    z_arrived(3)
    for i, peer in enumerate(one_peers):
        arrived(got_one.at[i], s_sem, (i,), peer)
    tot_two[...] = tot_one[...] + jnp.sum(got_one[...], axis=0)
    for i, peer in enumerate(two_peers):
        start(remote(tot_two, got_two.at[i], s_sem, (7 + i,), peer))
    y_forward(0)
    z_arrived(2)
    y_forward(1)
    y_forward(3)
    for i, peer in enumerate(two_peers):
        arrived(got_two.at[i], s_sem, (7 + i,), peer)
    tot_three[...] = tot_two[...] + jnp.sum(got_two[...], axis=0)
    for i, peer in enumerate(three_peers):
        start(remote(tot_three, got_three.at[i], s_sem, (14 + i,), peer))
    y_finish(0)
    y_forward(2)
    y_finish(1)
    y_finish(3)
    y_finish(2)
    for i, peer in enumerate(three_peers):
        arrived(got_three.at[i], s_sem, (14 + i,), peer)
    spread_out[...] = tot_three[...] + jnp.sum(got_three[...], axis=0)
    for q in range(4):
        there = gathered.at[pl.ds(block(q, 0, 1 - c), 2)]
        arrived(there, ac_sem, (0, q), other)
        there = gathered.at[pl.ds(block(q, 3, 1 - c), 2)]
        arrived(there, ac_sem, (1, q), other)
        there = gathered.at[pl.ds(block(q, 1, 1 - c), 2)]
        arrived(there, ac_sem, (2, q), other)
        there = gathered.at[pl.ds(block(q, 2, 1 - c), 1)]
        arrived(there, ac_sem, (3, q), other)
        there = gathered.at[pl.ds(block(q, 2, 1 - c) + 1, 1)]
        arrived(there, ac_sem, (4, q), other)
    for copy in sends:
        copy.wait_send()


def weight_kernel(
    count, offs, owners, basis_in, tall_in, gathered, sums, avg_in, sq_in, mom_in, w_in,
    w_out, mom_out, avg_out, sq_out, scales, inverse,
):
    step = pl.program_id(0)
    n_slots = gathered.shape[0]
    per = n_slots // CHUNKS

    @pl.when(step == 0)
    def _():
        spreads = []
        for s in range(STEPS):
            total = jnp.sum(sums[s], axis=(0, 1), keepdims=True)
            spread = jnp.sqrt(total * (1.0 / count) + rms_eps)
            scales[s] = jnp.sum(spread)
            spreads.append(spread)

        def body(i, _):
            part = gathered[pl.ds(i * per, per)]
            value = part[:, 0].astype(F32) / spreads[0][None] + part[:, 1].astype(F32) / spreads[1][None]
            out = dot(wide_lhs(value.reshape(per * BAND, BLOCK)), tall_in[...])
            inverse[pl.ds(i * per, per)] = out.reshape(per, BAND, BLOCK)
            return 0

        lax.fori_loop(0, CHUNKS, body, 0)
        avg_out[...] = avg_in[...]
        sq_out[...] = sq_in[...]

    mom_out[...] = mom_in[...]
    for i in range(per):
        j = step * per + i
        cols = slice(i * BLOCK, (i + 1) * BLOCK)
        rows = basis_in[pl.ds(offs[j], BAND), :]
        change = project_back(rows, inverse[owners[j]])
        w_out[:, cols] = (w_in[:, cols].astype(F32) - learning_rate * change).astype(BF16)


def per_device(weights, momentum, grads, offsets, owners, exp_avg, exp_sq):
    n_cb = offsets.shape[1]
    rows, cols = weights.shape
    table = dct_table(BLOCK)
    basis = jnp.asarray(table)
    offs, own = offsets[0], owners[0]
    index = jnp.arange(n_cb, dtype=jnp.int32)
    order = jnp.sum(jnp.where(own[:, None] == index[None, :], index[:, None], 0), axis=0)
    vmem, smem, hbm = (
        pl.BlockSpec(memory_space=s) for s in (pltpu.VMEM, pltpu.SMEM, pl.ANY)
    )
    piece = (STEPS, BAND, BLOCK)
    like = jax.ShapeDtypeStruct
    mom, gathered, avg, sq, sums = pl.pallas_call(
        main_kernel,
        out_shape=(
            like(momentum.shape, BF16),
            like((n_cb,) + piece, BF16),
            like(exp_avg.shape, F32),
            like(exp_sq.shape, F32),
            like((STEPS, 8, BLOCK), F32),
        ),
        in_specs=[smem, smem, vmem, vmem, hbm, hbm, vmem, vmem],
        out_specs=(vmem,) * 5,
        scratch_shapes=[
            pltpu.VMEM((CHUNKS, rows, cols // CHUNKS), BF16),
            pltpu.VMEM((STEPS, CHUNKS, rows, cols // CHUNKS), BF16),
            pltpu.VMEM((n_cb,) + piece, F32),
            pltpu.VMEM((n_cb,) + piece, BF16),
            pltpu.VMEM((4, 2, 4) + piece, BF16),
            pltpu.VMEM((4, 2, 4) + piece, BF16),
            pltpu.VMEM((3, 2, 4) + piece, BF16),
            pltpu.VMEM((2, 4) + piece, BF16),
            pltpu.VMEM((2, 2, 4) + piece, BF16),
            pltpu.VMEM((3, 2) + piece, BF16),
            pltpu.VMEM((3, 2) + piece, BF16),
            pltpu.VMEM((2, 4) + piece, F32),
            pltpu.VMEM((STEPS, 8, BLOCK), F32),
            pltpu.VMEM((STEPS, 8, BLOCK), F32),
            pltpu.VMEM((STEPS, 8, BLOCK), F32),
            pltpu.VMEM((7, STEPS, 8, BLOCK), F32),
            pltpu.VMEM((7, STEPS, 8, BLOCK), F32),
            pltpu.VMEM((3, STEPS, 8, BLOCK), F32),
            pltpu.SemaphoreType.DMA((3, CHUNKS)),
            pltpu.SemaphoreType.DMA((2, 4)),
            pltpu.SemaphoreType.DMA((2, 6, 4)),
            pltpu.SemaphoreType.DMA((2, 3)),
            pltpu.SemaphoreType.DMA((2, 3)),
            pltpu.SemaphoreType.DMA((2, 4, 4)),
            pltpu.SemaphoreType.DMA((2, 5, 4)),
            pltpu.SemaphoreType.DMA((2, 17)),
        ],
        compiler_params=pltpu.CompilerParams(
            collective_id=0, has_side_effects=True, vmem_limit_bytes=40 * 1024 * 1024
        ),
        name="bands",
    )(offs, order, basis, jnp.asarray(tall(table.T)), momentum, grads, exp_avg, exp_sq)

    count = float(exp_avg.size * lax.axis_size(WIDE) * lax.axis_size(SHARD))
    width = cols // CHUNKS
    slab = pl.BlockSpec((rows, width), lambda i: (0, i))
    slab3 = pl.BlockSpec((1, rows, width), lambda i: (0, 0, i))
    new_weights, new_momentum, new_avg, new_sq, scales = pl.pallas_call(
        functools.partial(weight_kernel, count),
        grid=(CHUNKS,),
        out_shape=(
            like(weights.shape, BF16),
            like(momentum.shape, BF16),
            like(exp_avg.shape, F32),
            like(exp_sq.shape, F32),
            like((STEPS,), F32),
        ),
        in_specs=[smem, smem, vmem, vmem, vmem, vmem, vmem, vmem, slab3, slab],
        out_specs=(slab, slab3, vmem, vmem, smem),
        scratch_shapes=[pltpu.VMEM((n_cb, BAND, BLOCK), F32)],
        compiler_params=pltpu.CompilerParams(
            dimension_semantics=("arbitrary",), vmem_limit_bytes=24 * 1024 * 1024
        ),
        name="weights",
    )(offs, own, basis, jnp.asarray(tall(table)), gathered, sums, avg, sq, mom, weights)
    return new_weights, new_momentum, new_avg, new_sq, scales


def solution(mesh):
    split_mesh = Mesh(mesh.devices.reshape(4, 4, 2, 2, 4), ("zh", "y", "c", "zl", "x"))
    in_specs = (
        P(SHARD, None),
        P(WIDE, SHARD, None),
        P(None, WIDE, SHARD, None),
        P(SHARD, None),
        P(SHARD, None),
        P(SHARD, WIDE, None, None),
        P(SHARD, WIDE, None, None),
    )
    out_specs = (
        P(SHARD, None),
        P(WIDE, SHARD, None),
        P(SHARD, WIDE, None, None),
        P(SHARD, WIDE, None, None),
        P(),
    )
    return jax.shard_map(
        per_device, mesh=split_mesh, in_specs=in_specs, out_specs=out_specs, check_vma=False
    )
```

```python
import functools

import jax
import jax.numpy as jnp
import numpy as np
from jax import lax
from jax.experimental import pallas as pl
from jax.experimental.pallas import tpu as pltpu
from jax.sharding import Mesh
from jax.sharding import PartitionSpec as P

STEPS = 2
BLOCK = 128
BAND = 32
CHUNKS = 8
WIDE = ("zh", "y", "c")
SHARD = ("zl", "x")
MESH = pl.DeviceIdType.MESH
F32 = jnp.float32
BF16 = jnp.bfloat16

momentum_decay = 0.9
beta_one = 0.8
beta_two = 0.95
adam_eps = 1e-08
rms_eps = 1e-06
learning_rate = 0.2


def dct_table(length):
    k = np.arange(length, dtype=np.float64)[:, None]
    n = np.arange(length, dtype=np.float64)[None, :]
    table = np.cos(np.pi * (2.0 * n + 1.0) * k / (2.0 * length))
    return (table * np.where(k == 0.0, np.sqrt(1.0 / length), np.sqrt(2.0 / length))).astype(np.float32)


def split(value):
    high = value.astype(BF16)
    return high, (value - high.astype(F32)).astype(BF16)


def tall(table):
    high = table.astype(BF16)
    low = (table - high.astype(np.float32)).astype(BF16)
    return np.concatenate([high, high, low], axis=0)


def wide_lhs(value):
    high, low = split(value)
    return jnp.concatenate([high, low, high], axis=-1)


def dot(a, b):
    return jnp.dot(a, b, preferred_element_type=F32)


def four_rows(rows):
    high, low = split(rows)
    return jnp.concatenate([high, low, high, low], axis=0)


def four_coefs(coefs):
    high, low = split(coefs)
    return jnp.concatenate([high, high, low, low], axis=0)


def main_kernel(
    offs_hbm, owners_hbm, basis_hbm, tall_hbm, back_hbm, mom_in, grad_in, avg_hbm, sq_hbm,
    mom_out, gathered, turned, avg_out, sq_out, spread_out,
    offs_vec, order_vec, offs_mem, order_mem, basis_in, tall_in, back_in, avg_in, sq_in,
    mbuf, gbuf, left, band, csend, crecv, ysend, yone, ytwo, zsend, zrecv, own,
    tot_one, tot_two, got_one, got_two,
    small_sem, load_sem, c_sem, y_sem, z_sem, az_sem, ay_sem, ac_sem, s_sem,
):
    zh, y, c = lax.axis_index("zh"), lax.axis_index("y"), lax.axis_index("c")
    zl, x = lax.axis_index("zl"), lax.axis_index("x")
    n_cb = left.shape[0]
    per = n_cb // CHUNKS
    y_up, y_down = {"y": lax.rem(y + 1, 4)}, {"y": lax.rem(y + 3, 4)}
    other = {"c": 1 - c}

    def zh_at(q):
        return {"zh": lax.rem(zh + q, 4)}

    one_peers = [
        {"x": lax.rem(x + i, 4), "y": lax.rem(y + j, 4)} for i in (2, 1, 3, 0) for j in (2, 1, 3, 0) if i or j
    ]
    two_peers = [
        {"c": lax.rem(c + i, 2), "zh": lax.rem(zh + q, 4), "zl": lax.rem(zl + j, 2)}
        for q in (2, 1, 3, 0) for j in range(2) for i in range(2) if q or i or j
    ]

    def load(chunk):
        cols = pl.ds(pl.multiple_of(chunk * (per * BLOCK), 128), per * BLOCK)
        return (
            pltpu.make_async_copy(mom_in.at[0, :, cols], mbuf.at[chunk], load_sem.at[0, chunk]),
            pltpu.make_async_copy(grad_in.at[0, 0, :, cols], gbuf.at[0, chunk], load_sem.at[1, chunk]),
            pltpu.make_async_copy(grad_in.at[1, 0, :, cols], gbuf.at[1, chunk], load_sem.at[2, chunk]),
        )

    def start_load(chunk, _):
        for copy in load(chunk):
            copy.start()
        return 0

    small = [
        pltpu.make_async_copy(src, dst, small_sem.at[i])
        for i, (src, dst) in enumerate(
            [
                (owners_hbm, offs_vec),
                (offs_hbm, offs_mem),
                (basis_hbm, basis_in),
                (tall_hbm, tall_in),
                (avg_hbm, avg_in),
                (sq_hbm, sq_in),
                (back_hbm, back_in),
            ]
        )
    ]
    for copy in small[:4]:
        copy.start()
    lax.fori_loop(0, CHUNKS, start_load, 0)
    for copy in small[4:]:
        copy.start()

    barrier = pltpu.get_barrier_semaphore()
    everyone = one_peers + two_peers
    for peer in everyone:
        pl.semaphore_signal(barrier, inc=1, device_id=peer, device_id_type=MESH)

    small[0].wait()
    owner = jnp.concatenate([offs_vec[...], jnp.full((1, BLOCK - n_cb), BLOCK, jnp.int32)], axis=1)
    owner = jnp.transpose(jnp.broadcast_to(owner, (BLOCK, BLOCK)))
    lane = lax.broadcasted_iota(jnp.int32, (BLOCK, BLOCK), 1)
    row = lax.broadcasted_iota(jnp.int32, (BLOCK, BLOCK), 0)
    order_vec[...] = jnp.max(jnp.where(owner == lane, row, 0), axis=0, keepdims=True)
    to_order = pltpu.make_async_copy(order_vec, order_mem, small_sem.at[7])
    to_order.start()
    for copy in small[1:4]:
        copy.wait()

    def bands(chunk, _):
        for copy in load(chunk):
            copy.wait()
        for i in range(per):
            j = chunk * per + i
            cols = slice(i * BLOCK, (i + 1) * BLOCK)
            rows = basis_in[pl.ds(offs_mem[0, j], BAND), :]
            both = jnp.concatenate(split(rows), axis=0)
            m = dot(both, mbuf[chunk, :, cols])
            g = dot(both, gbuf[0, chunk, :, cols])
            h = dot(both, gbuf[1, chunk, :, cols])
            left[j, 0] = momentum_decay * (m[:BAND] + m[BAND:]) + (g[:BAND] + g[BAND:])
            left[j, 1] = h[:BAND] + h[BAND:]
        value = left[pl.ds(chunk * per, per)].reshape(per * STEPS * BAND, BLOCK)
        out = dot(wide_lhs(value), tall_in[...])
        band[pl.ds(chunk * per, per)] = out.astype(BF16).reshape(per, STEPS, BAND, BLOCK)
        return 0

    lax.fori_loop(0, CHUNKS, bands, 0)
    to_order.wait()

    def slot(r, k, q, core):
        return lax.rem(zh + q, 4) * 16 + lax.rem(y + r, 4) * 4 + core * 2 + k

    def pack(r):
        def body(i, _):
            k, q = i // 4, lax.rem(i, 4)
            csend[r, k, q] = band[order_mem[0, slot(r, k, q, 1 - c)]]
            return 0

        lax.fori_loop(0, 8, body, 0)

    def remote(src, dst, sems, index, peer):
        return pltpu.make_async_remote_copy(
            src_ref=src, dst_ref=dst, send_sem=sems.at[(0,) + index], recv_sem=sems.at[(1,) + index],
            device_id=peer, device_id_type=MESH,
        )

    sends = []

    def start(copy):
        copy.start()
        sends.append(copy)
        return copy

    ranks = (2, 1, 3, 0)
    c_copies = {}
    pack(2)
    pl.semaphore_wait(barrier, len(everyone))
    for r in ranks:
        if r != 2:
            pack(r)
        c_copies[r] = start(remote(csend.at[r], crecv.at[r], c_sem, (r,), other))

    def merge(r):
        def body(i, _):
            k, q = i // 4, lax.rem(i, 4)
            total = band[order_mem[0, slot(r, k, q, c)]].astype(F32) + crecv[r, k, q].astype(F32)
            if r == 0:
                own[k, q] = total
            else:
                ysend[r - 1, k, q] = total.astype(BF16)
            return 0

        lax.fori_loop(0, 8, body, 0)

    q_order = (2, 1, 3, 0)
    c_copies[2].wait_recv()
    merge(2)
    first, early, late = {}, {}, {}
    for q in q_order:
        first[0, q] = start(remote(ysend.at[1, 0, q], yone.at[0, q], y_sem, (0, q), y_up))
        first[1, q] = start(remote(ysend.at[1, 1, q], yone.at[1, q], y_sem, (1, q), y_down))
    c_copies[1].wait_recv()
    merge(1)
    c_copies[3].wait_recv()
    merge(3)

    def start_early(q):
        early[0, q] = start(remote(ysend.at[0, 1, q], ytwo.at[0, 1, q], y_sem, (2, q), y_up))
        early[1, q] = start(remote(ysend.at[2, 0, q], ytwo.at[1, 0, q], y_sem, (3, q), y_down))

    def start_late(q):
        first[0, q].wait_recv()
        ysend[0, 0, q] = (ysend[0, 0, q].astype(F32) + yone[0, q].astype(F32)).astype(BF16)
        late[0, q] = start(remote(ysend.at[0, 0, q], ytwo.at[0, 0, q], y_sem, (4, q), y_up))
        first[1, q].wait_recv()
        ysend[2, 1, q] = (ysend[2, 1, q].astype(F32) + yone[1, q].astype(F32)).astype(BF16)
        late[1, q] = start(remote(ysend.at[2, 1, q], ytwo.at[1, 1, q], y_sem, (5, q), y_down))

    start_early(2)
    start_early(1)
    c_copies[0].wait_recv()
    merge(0)
    start_late(2)
    start_early(3)
    start_late(1)
    start_early(0)
    start_late(3)
    start_late(0)

    def momenta(chunk, _):
        for i in range(per):
            j = chunk * per + i
            cols = slice(i * BLOCK, (i + 1) * BLOCK)
            back = jnp.transpose(four_rows(basis_in[pl.ds(offs_mem[0, j], BAND), :]))
            turned[j] = back
            lost = dot(back, four_coefs(momentum_decay * left[j, 0] + left[j, 1]))
            blended = momentum_decay * mbuf[chunk, :, cols].astype(F32) + gbuf[0, chunk, :, cols].astype(F32)
            blended = momentum_decay * blended + gbuf[1, chunk, :, cols].astype(F32)
            where = pl.ds(pl.multiple_of(j * BLOCK, 128), BLOCK)
            mom_out[0, :, where] = (blended - lost).astype(BF16)
        return 0

    lax.fori_loop(0, CHUNKS // 2, momenta, 0)

    z_copies = {}
    for q in q_order:
        for copies in (early, late):
            copies[0, q].wait_recv()
            copies[1, q].wait_recv()
        for k in range(2):
            total = own[k, q] + ytwo[0, k, q].astype(F32) + ytwo[1, k, q].astype(F32)
            if q == 0:
                own[k, 0] = total
            else:
                zsend[q - 1, k] = total.astype(BF16)
        if q != 0:
            z_copies[q] = start(remote(zsend.at[q - 1], zrecv.at[q - 1], z_sem, (q - 1,), zh_at(q)))

    lax.fori_loop(CHUNKS // 2, CHUNKS, momenta, 0)

    for q in (1, 3, 2):
        z_copies[q].wait_recv()
    for copy in small[4:]:
        copy.wait()
    base = zh * 16 + y * 4 + c * 2
    replicas = lax.axis_size("zh") * lax.axis_size("y") * lax.axis_size("c")
    raws = []
    sums = [jnp.zeros((1, BLOCK), F32)] * STEPS
    for k in range(2):
        mean = own[k, 0] + zrecv[0, k].astype(F32) + zrecv[1, k].astype(F32) + zrecv[2, k].astype(F32)
        mean = mean * (1.0 / replicas)
        avg, sq = avg_in[0, k], sq_in[0, k]
        for step in range(STEPS):
            avg = beta_one * avg + (1.0 - beta_one) * mean[step]
            sq = beta_two * sq + (1.0 - beta_two) * mean[step] * mean[step]
            raw = avg / (jnp.sqrt(sq) + adam_eps)
            sums[step] += jnp.sum(raw * raw, axis=0, keepdims=True)
            raws.append(raw)
        avg_out[0, k] = avg
        sq_out[0, k] = sq
    spatial = dot(wide_lhs(jnp.concatenate(raws, axis=0)), back_in[...])
    gathered[pl.ds(base, 2)] = spatial.astype(BF16).reshape(2, STEPS, BAND, BLOCK)
    tot_one[...] = jnp.concatenate(sums, axis=0)

    def one(q, r, core, k):
        return gathered.at[lax.rem(zh + q, 4) * 16 + lax.rem(y + r, 4) * 4 + core * 2 + k]

    def share(view, sems, index, peer):
        start(remote(view, view, sems, index, peer))

    def arrived(view, sems, index, peer):
        remote(view, view, sems, index, peer).wait_recv()

    for q in (2, 1, 3):
        for k in range(2):
            share(one(0, 0, c, k), az_sem, (q - 1, k), zh_at(q))

    def y_start(q):
        for k in range(2):
            share(one(q, 0, c, k), ay_sem, (0, q, k), y_up)
            share(one(q, 0, c, 1 - k), ay_sem, (1, q, 1 - k), y_down)
        for k in range(2):
            share(one(q, 0, c, k), ac_sem, (0, q, k), other)

    def y_forward(q):
        arrived(one(q, 3, c, 0), ay_sem, (0, q, 0), y_up)
        share(one(q, 3, c, 0), ay_sem, (2, q, 0), y_up)
        share(one(q, 3, c, 0), ac_sem, (3, q, 0), other)
        arrived(one(q, 1, c, 1), ay_sem, (1, q, 1), y_down)
        share(one(q, 1, c, 1), ay_sem, (2, q, 1), y_down)
        share(one(q, 1, c, 1), ac_sem, (1, q, 1), other)
        arrived(one(q, 3, c, 1), ay_sem, (0, q, 1), y_up)
        share(one(q, 3, c, 1), ac_sem, (3, q, 1), other)
        arrived(one(q, 1, c, 0), ay_sem, (1, q, 0), y_down)
        share(one(q, 1, c, 0), ac_sem, (1, q, 0), other)

    def y_finish(q):
        arrived(one(q, 2, c, 0), ay_sem, (2, q, 0), y_up)
        share(one(q, 2, c, 0), ac_sem, (2, q, 0), other)
        arrived(one(q, 2, c, 1), ay_sem, (2, q, 1), y_down)
        share(one(q, 2, c, 1), ac_sem, (2, q, 1), other)

    def z_arrived(q):
        for k in range(2):
            arrived(one(q, 0, c, k), az_sem, (4 - q - 1, k), zh_at(q))
        y_start(q)

    y_start(0)
    for i, peer in enumerate(one_peers):
        start(remote(tot_one, got_one.at[i], s_sem, (i,), peer))
    y_forward(0)
    z_arrived(1)
    z_arrived(3)
    total = tot_one[...]
    for i, peer in enumerate(one_peers):
        arrived(got_one.at[i], s_sem, (i,), peer)
        total += got_one[i]
    tot_two[...] = total
    for i, peer in enumerate(two_peers):
        start(remote(tot_two, got_two.at[i], s_sem, (15 + i,), peer))
    z_arrived(2)
    y_finish(0)
    y_forward(1)
    y_forward(3)
    y_forward(2)
    y_finish(1)
    y_finish(3)
    y_finish(2)
    for i, peer in enumerate(two_peers):
        arrived(got_two.at[i], s_sem, (15 + i,), peer)
        total += got_two[i]
    spread_out[...] = total
    for q in range(4):
        for r in range(4):
            for k in range(2):
                arrived(one(q, r, 1 - c, k), ac_sem, (r, q, k), other)
    for copy in sends:
        copy.wait_send()


def weight_kernel(
    count, owners, gathered, turned, sums, avg_in, sq_in, mom_in, w_in,
    w_out, mom_out, avg_out, sq_out, scales, buffer, out_sem, same_sem,
):
    n_slots = gathered.shape[0]
    per = n_slots // CHUNKS
    same = [
        pltpu.make_async_copy(src, dst, same_sem.at[i])
        for i, (src, dst) in enumerate([(mom_in, mom_out), (avg_in, avg_out), (sq_in, sq_out)])
    ]
    for copy in same:
        copy.start()
    parts = []
    for s in range(STEPS):
        total = jnp.sum(sums[s : s + 1], axis=1, keepdims=True)
        spread = jnp.sqrt(total * (1.0 / count) + rms_eps)
        scales[s] = jnp.sum(spread)
        parts.append(-learning_rate / spread)

    def store(chunk):
        cols = pl.ds(pl.multiple_of(chunk * (per * BLOCK), 128), per * BLOCK)
        return pltpu.make_async_copy(buffer.at[:, cols], w_out.at[:, cols], out_sem.at[chunk])

    def body(chunk, _):
        for i in range(per):
            j = chunk * per + i
            pair = gathered[owners[0, j]]
            change = dot(turned[j], four_coefs(pair[0].astype(F32) * parts[0] + pair[1].astype(F32) * parts[1]))
            cols = pl.ds(pl.multiple_of(j * BLOCK, 128), BLOCK)
            buffer[:, cols] = (w_in[:, cols].astype(F32) + change).astype(BF16)
        store(chunk).start()
        return 0

    lax.fori_loop(0, CHUNKS, body, 0)

    def drain(chunk, _):
        store(chunk).wait()
        return 0

    lax.fori_loop(0, CHUNKS, drain, 0)
    for copy in same:
        copy.wait()


def per_device(weights, momentum, grads, offsets, owners, exp_avg, exp_sq):
    n_cb = offsets.shape[1]
    rows, cols = weights.shape
    table = dct_table(BLOCK)
    basis = jnp.asarray(table)
    vmem, smem, hbm = (
        pl.BlockSpec(memory_space=s) for s in (pltpu.VMEM, pltpu.SMEM, pltpu.HBM)
    )
    piece = (STEPS, BAND, BLOCK)
    like = jax.ShapeDtypeStruct
    mom, gathered, turned, avg, sq, sums = pl.pallas_call(
        main_kernel,
        out_shape=(
            like(momentum.shape, BF16),
            like((n_cb,) + piece, BF16),
            like((n_cb, BLOCK, BLOCK), BF16),
            like(exp_avg.shape, F32),
            like(exp_sq.shape, F32),
            like((STEPS, BLOCK), F32),
        ),
        in_specs=[hbm] * 9,
        out_specs=(vmem,) * 6,
        scratch_shapes=[
            pltpu.VMEM((1, n_cb), jnp.int32),
            pltpu.VMEM((1, BLOCK), jnp.int32),
            pltpu.SMEM((1, n_cb), jnp.int32),
            pltpu.SMEM((1, BLOCK), jnp.int32),
            pltpu.VMEM((BLOCK, BLOCK), F32),
            pltpu.VMEM((3 * BLOCK, BLOCK), BF16),
            pltpu.VMEM((3 * BLOCK, BLOCK), BF16),
            pltpu.VMEM(exp_avg.shape, F32),
            pltpu.VMEM(exp_sq.shape, F32),
            pltpu.VMEM((CHUNKS, rows, cols // CHUNKS), BF16),
            pltpu.VMEM((STEPS, CHUNKS, rows, cols // CHUNKS), BF16),
            pltpu.VMEM((n_cb,) + piece, F32),
            pltpu.VMEM((n_cb,) + piece, BF16),
            pltpu.VMEM((4, 2, 4) + piece, BF16),
            pltpu.VMEM((4, 2, 4) + piece, BF16),
            pltpu.VMEM((3, 2, 4) + piece, BF16),
            pltpu.VMEM((2, 4) + piece, BF16),
            pltpu.VMEM((2, 2, 4) + piece, BF16),
            pltpu.VMEM((3, 2) + piece, BF16),
            pltpu.VMEM((3, 2) + piece, BF16),
            pltpu.VMEM((2, 4) + piece, F32),
            pltpu.VMEM((STEPS, BLOCK), F32),
            pltpu.VMEM((STEPS, BLOCK), F32),
            pltpu.VMEM((15, STEPS, BLOCK), F32),
            pltpu.VMEM((15, STEPS, BLOCK), F32),
            pltpu.SemaphoreType.DMA((8,)),
            pltpu.SemaphoreType.DMA((3, CHUNKS)),
            pltpu.SemaphoreType.DMA((2, 4)),
            pltpu.SemaphoreType.DMA((2, 6, 4)),
            pltpu.SemaphoreType.DMA((2, 3)),
            pltpu.SemaphoreType.DMA((2, 3, 2)),
            pltpu.SemaphoreType.DMA((2, 3, 4, 2)),
            pltpu.SemaphoreType.DMA((2, 4, 4, 2)),
            pltpu.SemaphoreType.DMA((2, 30)),
        ],
        compiler_params=pltpu.CompilerParams(
            collective_id=0, has_side_effects=True, vmem_limit_bytes=40 * 1024 * 1024
        ),
        name="bands",
    )(
        *(
            pltpu.with_memory_space_constraint(array, pltpu.HBM)
            for array in (
                offsets, owners, basis, jnp.asarray(tall(table.T)), jnp.asarray(tall(table)), momentum, grads, exp_avg, exp_sq
            )
        )
    )

    count = float(exp_avg.size * lax.axis_size(WIDE) * lax.axis_size(SHARD))
    anywhere = pl.BlockSpec(memory_space=pl.ANY)
    new_weights, new_momentum, new_avg, new_sq, scales = pl.pallas_call(
        functools.partial(weight_kernel, count),
        out_shape=(
            like(weights.shape, BF16),
            like(momentum.shape, BF16),
            like(exp_avg.shape, F32),
            like(exp_sq.shape, F32),
            like((STEPS,), F32),
        ),
        in_specs=[smem] + [vmem] * 7,
        out_specs=(anywhere,) * 4 + (smem,),
        scratch_shapes=[
            pltpu.VMEM(weights.shape, BF16),
            pltpu.SemaphoreType.DMA((CHUNKS,)),
            pltpu.SemaphoreType.DMA((3,)),
        ],
        compiler_params=pltpu.CompilerParams(vmem_limit_bytes=24 * 1024 * 1024),
        name="weights",
    )(owners, gathered, turned, sums, avg, sq, mom, weights)
    return new_weights, new_momentum, new_avg, new_sq, scales


def solution(mesh):
    split_mesh = Mesh(mesh.devices.reshape(4, 4, 2, 2, 4), ("zh", "y", "c", "zl", "x"))
    in_specs = (
        P(SHARD, None),
        P(WIDE, SHARD, None),
        P(None, WIDE, SHARD, None),
        P(SHARD, None),
        P(SHARD, None),
        P(SHARD, WIDE, None, None),
        P(SHARD, WIDE, None, None),
    )
    out_specs = (
        P(SHARD, None),
        P(WIDE, SHARD, None),
        P(SHARD, WIDE, None, None),
        P(SHARD, WIDE, None, None),
        P(),
    )
    return jax.shard_map(
        per_device, mesh=split_mesh, in_specs=in_specs, out_specs=out_specs, check_vma=False
    )
```
